32 devices in a mesh: rep: 32 (over z, y, x, core).
Axes of the slice: x: 2, y: 2, z: 4, core: 2. Of those that a mesh axis runs over, the one named last changes fastest.
Arguments:
- inputs: bfloat16 [16384, 1024], P('rep'), may hold values from -6 to 6
- out_grads: bfloat16 [16384, 4096], P('rep'), may hold values from -0.29882812 to 0.29882812
- error_in: bfloat16 [32, 1024, 4096], P('rep'), may hold values from -6 to 6
- q_start: float32 [32, 4096], replicated, may hold values from -0.09375 to 0.09375
- master: float32 [1024, 4096], P(None, 'rep'), may hold values from -1.2 to 1.2
Outputs:
- error_out: bfloat16 [32, 1024, 4096], P('rep')
- q_out: float32 [32, 4096], replicated
- master_out: float32 [1024, 4096], P(None, 'rep')
The draws below stay inside these ranges and needn't reach their ends.
All inputs are finite; a program needn't handle non-finite values.
Results may differ from the reference program's by a relative error of at most 0.001.
Values sent between devices are 32-bit elements; how exact they have to be, the bound alone decides.
A program may use at most 128 MiB of HBM per device.

```python
import jax
import jax.numpy as jnp
from jax import lax

D = 1024
FF = 4096
RANK = 32
ITERS = 3
TOKENS = 16384
N_REP = 32


def steps_of(rng, shape, pieces, low, top_value):
    gain, own = 1.0, jax.random.fold_in(rng, 6)
    for position, parts in pieces:
        heights = jnp.exp(jax.random.uniform(jax.random.fold_in(own, position), (parts,), jnp.float32, low / len(pieces), top_value / len(pieces)))
        gain = gain * jnp.repeat(heights, shape[position] // parts).reshape([-1 if axis == position else 1 for axis in range(len(shape))])
    return gain


def gaussian(own_key, extent, spread, limit, pieces=(), held_as=jnp.bfloat16):
    result = jax.random.normal(own_key, extent, jnp.float32) * spread
    if len(pieces) > 0:
        result = steps_of(own_key, extent, pieces, -0.22, 0.18) * result
    return jnp.clip(result, min=-limit, max=limit).astype(held_as)


def setup_inputs(seed: int = 0) -> dict:
    splits = jax.random.split(jax.random.key(seed), 6)
    return {
        "inputs": gaussian(splits[0], (TOKENS, D), 1.0, 6.0, ((0, 32),)),
        "out_grads": gaussian(splits[1], (TOKENS, FF), 0.045, 0.29882812, ((0, 32),)),
        "error_in": gaussian(splits[2], (N_REP, D, FF), 1.0, 6.0, ((0, 32),)),
        "q_start": gaussian(splits[3], (RANK, FF), FF ** -0.5, 0.09375, (), jnp.float32),
        "master": gaussian(splits[4], (D, FF), 0.2, 1.2, ((1, 32),), jnp.float32),
    }


def orthonormal(rows):
    basis = jnp.zeros_like(rows)
    for k in range(rows.shape[0]):
        vector = rows[k]
        coef = jnp.dot(basis, vector, precision=lax.Precision.HIGHEST)
        vector = vector - jnp.dot(coef, basis, precision=lax.Precision.HIGHEST)
        basis = basis.at[k].set(vector / jnp.sqrt(jnp.sum(vector * vector) + 1.0))
    return basis

def reference(inputs, out_grads, error_in, q_start, master):
    tok = inputs.shape[0] // N_REP
    xs = inputs.reshape(N_REP, tok, inputs.shape[1])
    dys = out_grads.reshape(N_REP, tok, out_grads.shape[1])

    def one_replica(items):
        x_rows, dy_rows, error = items
        grad = lax.dot_general(x_rows, dy_rows, (((0,), (0,)), ((), ())), preferred_element_type=jnp.float32)
        return grad + error.astype(jnp.float32)
    merged = lax.map(one_replica, (xs, dys, error_in))
    merged_sum = lax.optimization_barrier(jnp.sum(merged, axis=0))
    factor = q_start
    basis = None
    for step in range(ITERS):
        p_total = lax.dot_general(factor, merged_sum, (((1,), (1,)), ((), ())), precision=lax.Precision.HIGHEST, preferred_element_type=jnp.float32)
        basis = orthonormal(p_total)
        factor = jnp.dot(basis, merged_sum, precision=lax.Precision.HIGHEST, preferred_element_type=jnp.float32) / N_REP
    recon = lax.dot_general(basis, factor, (((0,), (0,)), ((), ())), precision=lax.Precision.HIGHEST, preferred_element_type=jnp.float32)
    error_out = (merged - recon[None]).astype(jnp.bfloat16)
    master_out = master - 0.5 * recon
    return (error_out, factor, master_out)
```

```python
import functools

import jax
import jax.numpy as jnp
from jax import lax
from jax.experimental import pallas as pl
from jax.experimental.pallas import tpu as pltpu
from jax.sharding import PartitionSpec as P

ITERS = 3
AXIS = "rep"
MESH = pl.DeviceIdType.MESH
F32, BF16 = jnp.float32, jnp.bfloat16


def split_tiles(count, rows, cols):
    col_cuts = min(count, cols // 128)
    row_cuts = max(1, min(count // col_cuts, rows // 8))
    return row_cuts, col_cuts, count // (row_cuts * col_cuts)


def halves(value):
    high = value.astype(BF16)
    return high, (value - high.astype(F32)).astype(BF16)


def kernel(
    count, x_hbm, dy_hbm, err_hbm, start_ref, master_ref,
    err_out, q_out, master_out,
    x_v, xt_v, dy_v, m_hi, m_lo,
    q_full, q_part, q_recv, q_split, p_full, p_part, p_recv, vecs, basis, b_split, b_tall, p_tall,
    load_sem, dy_sem, err_sem,
    p_rs_send, p_rs_recv, p_ag_send, p_ag_recv, q_rs_send, q_rs_recv, q_ag_send, q_ag_recv,
):
    me = lax.axis_index(AXIS)
    err_v = err_out.at[0]
    rank, width = p_full.shape
    ff = q_full.shape[1]
    step_cols = dy_sem.shape[0]
    cw = ff // step_cols

    pltpu.make_async_copy(x_hbm, x_v, load_sem).start()
    for c in range(step_cols):
        cols = pl.ds(c * cw, cw)
        pltpu.make_async_copy(dy_hbm.at[:, cols], dy_v.at[:, cols], dy_sem.at[c]).start()
        pltpu.make_async_copy(err_hbm.at[0, :, cols], err_v.at[:, cols], err_sem.at[c]).start()

    barrier = pltpu.get_barrier_semaphore()

    @pl.loop(1, count)
    def _(d):
        pl.semaphore_signal(barrier, inc=1, device_id=(lax.rem(me + d, count),), device_id_type=MESH)

    def piece(cuts, shape, owner):
        row_cuts, col_cuts, stride = cuts
        index = owner // stride
        rows, cols = shape[0] // row_cuts, shape[1] // col_cuts
        row = pl.multiple_of((index % row_cuts) * rows, rows)
        col = pl.multiple_of((index // row_cuts) * cols, cols)
        return pl.ds(row, rows), pl.ds(col, cols)

    def is_owner(cuts, device):
        return lax.rem(device, cuts[2]) == 0

    def guarded(cuts, device, body):
        if cuts[2] == 1:
            body()
        else:
            pl.when(is_owner(cuts, device))(body)

    def send_piece(cuts, part, recv, send_sem, recv_sem, target):
        def body():
            pltpu.make_async_remote_copy(
                src_ref=part.at[piece(cuts, part.shape, target)],
                dst_ref=recv.at[lax.rem(target - me + count, count) - 1],
                send_sem=send_sem, recv_sem=recv_sem,
                device_id=(target,), device_id_type=MESH,
            ).start()
        guarded(cuts, target, body)

    def drain(recv, sem, pieces):
        if pieces:
            ref = recv.at[pl.ds(0, pieces)]
            pltpu.make_async_copy(ref, ref, sem).wait()

    def either(cuts, owner_body, other_body):
        if cuts[2] == 1:
            owner_body()
        else:
            pl.when(is_owner(cuts, me))(owner_body)
            pl.when(jnp.logical_not(is_owner(cuts, me)))(other_body)

    def add_up(cuts, part, full, recv, recv_sem, ag_send, ag_recv, scale):
        def body():
            mine = piece(cuts, part.shape, me)
            drain(recv, recv_sem, count - 1)
            total = part[mine] + jnp.sum(recv[...], axis=0)
            full[mine] = total if scale == 1 else total / scale

            @pl.loop(1, count)
            def _(d):
                pltpu.make_async_remote_copy(
                    src_ref=full.at[mine], dst_ref=full.at[mine],
                    send_sem=ag_send, recv_sem=ag_recv,
                    device_id=(lax.rem(me + d, count),), device_id_type=MESH,
                ).start()

        either(cuts, body, lambda: None)

    def drain_sends(cuts, recv, rs_send, ag_send):
        owners = cuts[0] * cuts[1]

        def owner_body():
            drain(recv, rs_send, owners - 1)
            drain(recv, ag_send, count - 1)

        either(cuts, owner_body, lambda: drain(recv, rs_send, owners))

    p_cuts = split_tiles(count, rank, width)
    q_cuts = split_tiles(count, rank, ff)
    q_width = ff // q_cuts[1]
    members = cw // q_width * q_cuts[0]
    own_group = me // q_cuts[2] // members

    def columns(group):
        return pl.ds(pl.multiple_of(group * cw, cw), cw)

    def await_group(group):
        either(
            q_cuts,
            lambda: own_or_other(group),
            lambda: drain(q_recv, q_ag_recv.at[group], members),
        )

    def own_or_other(group):
        @pl.when(group == own_group)
        def _():
            drain(q_recv, q_ag_recv.at[group], members - 1)

        @pl.when(group != own_group)
        def _():
            drain(q_recv, q_ag_recv.at[group], members)

    def absorb(source, cols):
        high, low = halves(source[:, cols])
        factor = jnp.concatenate([high, low], axis=0)
        dims = (((1,), (1,)), ((), ()))
        tall = lax.dot_general(m_hi[:, cols], factor, dims, preferred_element_type=F32)
        tall += lax.dot_general(m_lo[:, cols], factor, dims, preferred_element_type=F32)
        p_tall[...] += tall

    def settle():
        flat = p_tall[...].T
        p_part[...] = flat[0:rank] + flat[rank:2 * rank]
        p_tall[...] = jnp.zeros_like(p_tall)

    pltpu.make_async_copy(x_hbm, x_v, load_sem).wait()
    xt_v[...] = x_v[...].T
    p_tall[...] = jnp.zeros_like(p_tall)

    @pl.loop(0, step_cols)
    def _(c):
        cols = pl.ds(pl.multiple_of(c * cw, cw), cw)
        pltpu.make_async_copy(dy_hbm.at[:, cols], dy_v.at[:, cols], dy_sem.at[c]).wait()
        pltpu.make_async_copy(err_hbm.at[0, :, cols], err_v.at[:, cols], err_sem.at[c]).wait()
        merged = jnp.dot(xt_v[...], dy_v[:, cols], preferred_element_type=F32)
        high, low = halves(merged + err_v[:, cols].astype(F32))
        m_hi[:, cols] = high
        m_lo[:, cols] = low
        absorb(start_ref, cols)

    settle()
    pl.semaphore_wait(barrier, count - 1)

    @pl.loop(0, ITERS)
    def _(step):
        @pl.loop(1, count)
        def _(d):
            send_piece(p_cuts, p_part, p_recv, p_rs_send, p_rs_recv, lax.rem(me + d, count))

        add_up(p_cuts, p_part, p_full, p_recv, p_rs_recv, p_ag_send, p_ag_recv, 1)
        p_owners = p_cuts[0] * p_cuts[1]
        either(
            p_cuts,
            lambda: drain(p_recv, p_ag_recv, p_owners - 1),
            lambda: drain(p_recv, p_ag_recv, p_owners),
        )
        drain_sends(p_cuts, p_recv, p_rs_send, p_ag_send)

        vecs[...] = p_full[...]
        for base in range(0, rank, 8):
            block = pl.ds(base, 8)
            above, rest = p_full[block, :], vecs[block, :]
            done = []
            for k in range(8):
                row = rest[k:k + 1, :]
                norm = jnp.sum(row * row, axis=1, keepdims=True) + 1.0
                coef = jnp.sum(above * row, axis=1, keepdims=True)
                inverse = lax.rsqrt(norm)
                unit = row * inverse
                done.append(unit)
                if k < 7:
                    rest = rest - (coef * inverse) * unit
                for below in range(base + 8, rank, 8):
                    later = pl.ds(below, 8)
                    coef = jnp.sum(p_full[later, :] * unit, axis=1, keepdims=True)
                    vecs[later, :] = vecs[later, :] - coef * unit
            basis[block, :] = jnp.concatenate(done, axis=0)

        high, low = halves(basis[...])
        b_split[0:rank] = high
        b_split[rank:2 * rank] = low

        groups = ff // cw

        @pl.loop(0, groups)
        def _(i):
            group = lax.rem(own_group + 1 + i, groups)
            cols = pl.ds(pl.multiple_of(group * cw, cw), cw)
            both = jnp.dot(b_split[...], m_hi[:, cols], preferred_element_type=F32)
            both += jnp.dot(b_split[...], m_lo[:, cols], preferred_element_type=F32)
            q_part[:, cols] = both[0:rank] + both[rank:2 * rank]

            for j in range(members):
                target = (group * members + j) * q_cuts[2]

                @pl.when(target != me)
                def _():
                    pltpu.make_async_remote_copy(
                        src_ref=q_part.at[piece(q_cuts, q_part.shape, target)],
                        dst_ref=q_recv.at[lax.rem(target - me + count, count) - 1],
                        send_sem=q_rs_send, recv_sem=q_rs_recv,
                        device_id=(target,), device_id_type=MESH,
                    ).start()

        add_up(
            q_cuts, q_part, q_full, q_recv, q_rs_recv, q_ag_send, q_ag_recv.at[own_group], count
        )

        @pl.when(step < ITERS - 1)
        def _():
            @pl.loop(0, step_cols)
            def _(i):
                group = lax.rem(own_group - i + step_cols, step_cols)
                await_group(group)
                absorb(q_full, columns(group))

            drain_sends(q_cuts, q_recv, q_rs_send, q_ag_send)
            settle()

    tall = basis[...].T
    high, low = halves(tall)
    b_tall[:, 0:rank] = high
    b_tall[:, rank:2 * rank] = high
    b_tall[:, 2 * rank:3 * rank] = low

    @pl.loop(0, step_cols)
    def _(i):
        group = lax.rem(own_group - i + step_cols, step_cols)
        await_group(group)
        cols = columns(group)
        high, low = halves(q_full[:, cols])
        factor = jnp.concatenate([high, low, high], axis=0)
        q_split[:, cols] = factor
        recon = jnp.dot(b_tall[...], factor, preferred_element_type=F32)
        merged = m_hi[:, cols].astype(F32) + m_lo[:, cols].astype(F32)
        err_v[:, cols] = (merged - recon).astype(BF16)

    drain_sends(q_cuts, q_recv, q_rs_send, q_ag_send)
    q_out[...] = q_full[...]

    own = master_ref.shape[1]
    if own % 128 == 0:
        mine = q_split[:, pl.ds(pl.multiple_of(me * own, own), own)]
    else:
        base = pl.multiple_of((me * own) // 128 * 128, 128)
        block = q_split[:, pl.ds(base, 128)].astype(F32)
        shift = lax.rem(128 - lax.rem(me * own, 128), 128)
        mine = pltpu.roll(block, shift, 1)[:, 0:own].astype(BF16)
    master_out[...] = master_ref[...] - 0.5 * jnp.dot(b_tall[...], mine, preferred_element_type=F32)


def shards(inputs, out_grads, error_in, q_start, master):
    count = lax.axis_size(AXIS)
    tokens, width = inputs.shape
    ff = out_grads.shape[1]
    rank = q_start.shape[0]
    steps = ff // 512
    hbm_spec = pl.BlockSpec(memory_space=pltpu.HBM)
    vmem_spec = pl.BlockSpec(memory_space=pltpu.VMEM)
    p_cuts, q_cuts = split_tiles(count, rank, width), split_tiles(count, rank, ff)
    dma = pltpu.SemaphoreType.DMA
    return pl.pallas_call(
        functools.partial(kernel, count),
        out_shape=(
            pltpu.VMEM(error_in.shape, BF16),
            pltpu.VMEM(q_start.shape, F32),
            pltpu.VMEM(master.shape, F32),
        ),
        in_specs=[hbm_spec] * 3 + [vmem_spec] * 2,
        out_specs=(vmem_spec, vmem_spec, vmem_spec),
        scratch_shapes=[
            pltpu.VMEM((tokens, width), BF16),
            pltpu.VMEM((width, tokens), BF16),
            pltpu.VMEM((tokens, ff), BF16),
            pltpu.VMEM((width, ff), BF16),
            pltpu.VMEM((width, ff), BF16),
            pltpu.VMEM((rank, ff), F32),
            pltpu.VMEM((rank, ff), F32),
            pltpu.VMEM((count - 1, rank // q_cuts[0], ff // q_cuts[1]), F32),
            pltpu.VMEM((3 * rank, ff), BF16),
            pltpu.VMEM((rank, width), F32),
            pltpu.VMEM((rank, width), F32),
            pltpu.VMEM((count - 1, rank // p_cuts[0], width // p_cuts[1]), F32),
            pltpu.VMEM((rank, width), F32),
            pltpu.VMEM((rank, width), F32),
            pltpu.VMEM((2 * rank, width), BF16),
            pltpu.VMEM((width, 3 * rank), BF16),
            pltpu.VMEM((width, 2 * rank), F32),
            dma, dma((steps,)), dma((steps,)),
            dma, dma, dma, dma, dma, dma, dma, dma((steps,)),
        ],
        compiler_params=pltpu.CompilerParams(
            collective_id=0, has_side_effects=True, vmem_limit_bytes=44 * 1024 * 1024
        ),
    )(inputs, out_grads, error_in, q_start, master)


def solution(mesh):
    return jax.shard_map(
        shards,
        mesh=mesh,
        in_specs=(P("rep", None), P("rep", None), P("rep", None, None), P(), P(None, "rep")),
        out_specs=(P("rep", None, None), P(), P(None, "rep")),
        check_vma=False,
    )
```

```python
import functools

import jax
import jax.numpy as jnp
from jax import lax
from jax.experimental import pallas as pl
from jax.experimental.pallas import tpu as pltpu
from jax.sharding import PartitionSpec as P

ITERS = 3
AXIS = "rep"
MESH = pl.DeviceIdType.MESH
F32, BF16 = jnp.float32, jnp.bfloat16


def split_tiles(count, rows, cols):
    col_cuts = min(count, cols // 128)
    row_cuts = max(1, min(count // col_cuts, rows // 8))
    return row_cuts, col_cuts, count // (row_cuts * col_cuts)


def halves(value):
    high = value.astype(BF16)
    return high, (value - high.astype(F32)).astype(BF16)


def kernel(
    count, x_hbm, dy_hbm, err_hbm, start_ref, master_ref,
    err_out, q_out, master_out,
    x_v, xt_v, dy_v, m_hi, m_lo,
    q_full, q_part, q_recv, q_split, p_full, p_part, p_recv, vecs, basis, b_split, b_tall, p_tall,
    load_sem, dy_sem, err_sem,
    p_rs_send, p_rs_recv, p_ag_send, p_ag_recv, q_rs_send, q_rs_recv, q_ag_send, q_ag_recv,
):
    me = lax.axis_index(AXIS)
    err_v = err_out.at[0]
    rank, width = p_full.shape
    ff = q_full.shape[1]
    step_cols = dy_sem.shape[0]
    cw = ff // step_cols

    pltpu.make_async_copy(x_hbm, x_v, load_sem).start()
    for c in range(step_cols):
        cols = pl.ds(c * cw, cw)
        pltpu.make_async_copy(dy_hbm.at[:, cols], dy_v.at[:, cols], dy_sem.at[c]).start()
        pltpu.make_async_copy(err_hbm.at[0, :, cols], err_v.at[:, cols], err_sem.at[c]).start()

    barrier = pltpu.get_barrier_semaphore()

    @pl.loop(1, count)
    def _(d):
        pl.semaphore_signal(barrier, inc=1, device_id=(lax.rem(me + d, count),), device_id_type=MESH)

    def piece(cuts, shape, owner):
        row_cuts, col_cuts, stride = cuts
        index = owner // stride
        rows, cols = shape[0] // row_cuts, shape[1] // col_cuts
        row = pl.multiple_of((index % row_cuts) * rows, rows)
        col = pl.multiple_of((index // row_cuts) * cols, cols)
        return pl.ds(row, rows), pl.ds(col, cols)

    def is_owner(cuts, device):
        return lax.rem(device, cuts[2]) == 0

    def guarded(cuts, device, body):
        if cuts[2] == 1:
            body()
        else:
            pl.when(is_owner(cuts, device))(body)

    def after(d):
        device = me + d
        return jnp.where(device < count, device, device - count)

    def drain(recv, sem, pieces):
        if pieces:
            ref = recv.at[pl.ds(0, pieces)]
            pltpu.make_async_copy(ref, ref, sem).wait()

    def either(cuts, owner_body, other_body):
        if cuts[2] == 1:
            owner_body()
        else:
            pl.when(is_owner(cuts, me))(owner_body)
            pl.when(jnp.logical_not(is_owner(cuts, me)))(other_body)

    def add_up(cuts, part, full, recv, recv_sem, ag_send, ag_recv, scale):
        def body():
            mine = piece(cuts, part.shape, me)
            drain(recv, recv_sem, count - 1)
            total = part[mine] + jnp.sum(recv[...], axis=0)
            full[mine] = total if scale == 1 else total / scale

            @pl.loop(1, count)
            def _(d):
                pltpu.make_async_remote_copy(
                    src_ref=full.at[mine], dst_ref=full.at[mine],
                    send_sem=ag_send, recv_sem=ag_recv,
                    device_id=(after(d),), device_id_type=MESH,
                ).start()

        either(cuts, body, lambda: None)

    def drain_sends(cuts, recv, rs_send, ag_send):
        owners = cuts[0] * cuts[1]

        def owner_body():
            drain(recv, rs_send, owners - 1)
            drain(recv, ag_send, count - 1)

        either(cuts, owner_body, lambda: drain(recv, rs_send, owners))

    p_cuts = split_tiles(count, rank, width)
    q_cuts = split_tiles(count, rank, ff)
    q_width = ff // q_cuts[1]
    members = cw // q_width * q_cuts[0]
    own_group = me // q_cuts[2] // members

    def columns(group):
        return pl.ds(pl.multiple_of(group * cw, cw), cw)

    def await_group(group):
        either(
            q_cuts,
            lambda: own_or_other(group),
            lambda: drain(q_recv, q_ag_recv.at[group], members),
        )

    def own_or_other(group):
        @pl.when(group == own_group)
        def _():
            drain(q_recv, q_ag_recv.at[group], members - 1)

        @pl.when(group != own_group)
        def _():
            drain(q_recv, q_ag_recv.at[group], members)

    def absorb(source, cols):
        high, low = halves(source[:, cols])
        factor = jnp.concatenate([high, low], axis=0)
        dims = (((1,), (1,)), ((), ()))
        tall = lax.dot_general(m_hi[:, cols], factor, dims, preferred_element_type=F32)
        tall += lax.dot_general(m_lo[:, cols], factor, dims, preferred_element_type=F32)
        p_tall[...] += tall

    def settle():
        flat = p_tall[...].T
        p_part[...] = flat[0:rank] + flat[rank:2 * rank]

        @pl.loop(1, count)
        def _(d):
            target = after(d)

            def send():
                pltpu.make_async_remote_copy(
                    src_ref=p_part.at[piece(p_cuts, p_part.shape, target)],
                    dst_ref=p_recv.at[d - 1],
                    send_sem=p_rs_send, recv_sem=p_rs_recv,
                    device_id=(target,), device_id_type=MESH,
                ).start()

            guarded(p_cuts, target, send)

        p_tall[...] = jnp.zeros_like(p_tall)

    pltpu.make_async_copy(x_hbm, x_v, load_sem).wait()
    xt_v[...] = x_v[...].T
    p_tall[...] = jnp.zeros_like(p_tall)

    @pl.loop(0, step_cols)
    def _(c):
        cols = pl.ds(pl.multiple_of(c * cw, cw), cw)
        pltpu.make_async_copy(dy_hbm.at[:, cols], dy_v.at[:, cols], dy_sem.at[c]).wait()
        pltpu.make_async_copy(err_hbm.at[0, :, cols], err_v.at[:, cols], err_sem.at[c]).wait()
        merged = jnp.dot(xt_v[...], dy_v[:, cols], preferred_element_type=F32)
        high, low = halves(merged + err_v[:, cols].astype(F32))
        m_hi[:, cols] = high
        m_lo[:, cols] = low
        absorb(start_ref, cols)

    pl.semaphore_wait(barrier, count - 1)
    settle()

    @pl.loop(0, ITERS)
    def _(step):
        add_up(p_cuts, p_part, p_full, p_recv, p_rs_recv, p_ag_send, p_ag_recv, 1)
        p_owners = p_cuts[0] * p_cuts[1]
        either(
            p_cuts,
            lambda: drain(p_recv, p_ag_recv, p_owners - 1),
            lambda: drain(p_recv, p_ag_recv, p_owners),
        )

        vecs[...] = p_full[...]
        for base in range(0, rank, 8):
            block = pl.ds(base, 8)
            above, rest = p_full[block, :], vecs[block, :]
            done = []
            for k in range(8):
                row = rest[k:k + 1, :]
                norm = jnp.sum(row * row, axis=1, keepdims=True) + 1.0
                coef = jnp.sum(above * row, axis=1, keepdims=True)
                inverse = lax.rsqrt(norm)
                unit = row * inverse
                done.append(unit)
                if k < 7:
                    rest = rest - (coef * inverse) * unit
                for below in range(base + 8, rank, 8):
                    later = pl.ds(below, 8)
                    coef = jnp.sum(p_full[later, :] * unit, axis=1, keepdims=True)
                    vecs[later, :] = vecs[later, :] - coef * unit
            basis[block, :] = jnp.concatenate(done, axis=0)

        high, low = halves(basis[...])
        b_split[0:rank] = high
        b_split[rank:2 * rank] = low

        groups = ff // cw

        @pl.loop(0, groups)
        def _(i):
            group = lax.rem(own_group + 1 + i, groups)
            cols = pl.ds(pl.multiple_of(group * cw, cw), cw)
            both = jnp.dot(b_split[...], m_hi[:, cols], preferred_element_type=F32)
            both += jnp.dot(b_split[...], m_lo[:, cols], preferred_element_type=F32)
            q_part[:, cols] = both[0:rank] + both[rank:2 * rank]

            for j in range(members):
                target = (group * members + j) * q_cuts[2]

                @pl.when(target != me)
                def _():
                    pltpu.make_async_remote_copy(
                        src_ref=q_part.at[piece(q_cuts, q_part.shape, target)],
                        dst_ref=q_recv.at[lax.rem(target - me + count, count) - 1],
                        send_sem=q_rs_send, recv_sem=q_rs_recv,
                        device_id=(target,), device_id_type=MESH,
                    ).start()

        add_up(
            q_cuts, q_part, q_full, q_recv, q_rs_recv, q_ag_send, q_ag_recv.at[own_group], count
        )

        drain_sends(p_cuts, p_recv, p_rs_send, p_ag_send)

        @pl.when(step < ITERS - 1)
        def _():
            @pl.loop(0, step_cols)
            def _(i):
                group = lax.rem(own_group - i + step_cols, step_cols)
                await_group(group)
                absorb(q_full, columns(group))

            settle()
            drain_sends(q_cuts, q_recv, q_rs_send, q_ag_send)

    tall = basis[...].T
    high, low = halves(tall)
    b_tall[:, 0:rank] = high
    b_tall[:, rank:2 * rank] = high
    b_tall[:, 2 * rank:3 * rank] = low

    @pl.loop(0, step_cols)
    def _(i):
        group = lax.rem(own_group - i + step_cols, step_cols)
        await_group(group)
        cols = columns(group)
        high, low = halves(q_full[:, cols])
        factor = jnp.concatenate([high, low, high], axis=0)
        q_split[:, cols] = factor
        recon = jnp.dot(b_tall[...], factor, preferred_element_type=F32)
        merged = m_hi[:, cols].astype(F32) + m_lo[:, cols].astype(F32)
        err_v[:, cols] = (merged - recon).astype(BF16)

    drain_sends(q_cuts, q_recv, q_rs_send, q_ag_send)
    q_out[...] = q_full[...]

    own = master_ref.shape[1]
    if own % 128 == 0:
        mine = q_split[:, pl.ds(pl.multiple_of(me * own, own), own)]
    else:
        base = pl.multiple_of((me * own) // 128 * 128, 128)
        block = q_split[:, pl.ds(base, 128)].astype(F32)
        shift = lax.rem(128 - lax.rem(me * own, 128), 128)
        mine = pltpu.roll(block, shift, 1)[:, 0:own].astype(BF16)
    master_out[...] = master_ref[...] - 0.5 * jnp.dot(b_tall[...], mine, preferred_element_type=F32)


def shards(inputs, out_grads, error_in, q_start, master):
    count = lax.axis_size(AXIS)
    tokens, width = inputs.shape
    ff = out_grads.shape[1]
    rank = q_start.shape[0]
    steps = ff // 512
    hbm_spec = pl.BlockSpec(memory_space=pltpu.HBM)
    vmem_spec = pl.BlockSpec(memory_space=pltpu.VMEM)
    p_cuts, q_cuts = split_tiles(count, rank, width), split_tiles(count, rank, ff)
    dma = pltpu.SemaphoreType.DMA
    return pl.pallas_call(
        functools.partial(kernel, count),
        out_shape=(
            pltpu.VMEM(error_in.shape, BF16),
            pltpu.VMEM(q_start.shape, F32),
            pltpu.VMEM(master.shape, F32),
        ),
        in_specs=[hbm_spec] * 3 + [vmem_spec] * 2,
        out_specs=(vmem_spec, vmem_spec, vmem_spec),
        scratch_shapes=[
            pltpu.VMEM((tokens, width), BF16),
            pltpu.VMEM((width, tokens), BF16),
            pltpu.VMEM((tokens, ff), BF16),
            pltpu.VMEM((width, ff), BF16),
            pltpu.VMEM((width, ff), BF16),
            pltpu.VMEM((rank, ff), F32),
            pltpu.VMEM((rank, ff), F32),
            pltpu.VMEM((count - 1, rank // q_cuts[0], ff // q_cuts[1]), F32),
            pltpu.VMEM((3 * rank, ff), BF16),
            pltpu.VMEM((rank, width), F32),
            pltpu.VMEM((rank, width), F32),
            pltpu.VMEM((count - 1, rank // p_cuts[0], width // p_cuts[1]), F32),
            pltpu.VMEM((rank, width), F32),
            pltpu.VMEM((rank, width), F32),
            pltpu.VMEM((2 * rank, width), BF16),
            pltpu.VMEM((width, 3 * rank), BF16),
            pltpu.VMEM((width, 2 * rank), F32),
            dma, dma((steps,)), dma((steps,)),
            dma, dma, dma, dma, dma, dma, dma, dma((steps,)),
        ],
        compiler_params=pltpu.CompilerParams(
            collective_id=0, has_side_effects=True, vmem_limit_bytes=44 * 1024 * 1024
        ),
    )(inputs, out_grads, error_in, q_start, master)


def solution(mesh):
    return jax.shard_map(
        shards,
        mesh=mesh,
        in_specs=(P("rep", None), P("rep", None), P("rep", None, None), P(), P(None, "rep")),
        out_specs=(P("rep", None, None), P(), P(None, "rep")),
        check_vma=False,
    )
```
